128 devices in a mesh: expert: 4 (over x_lo, core), shard: 32 (over z, y, x_hi).
Axes of the slice: x: 4 (x_hi: 2, x_lo: 2; x = x_hi * 2 + x_lo), y: 4, z: 4, core: 2. Of those that a mesh axis runs over, the one named last changes fastest.
Arguments:
- master_gate: float32 [64, 2048, 1024], P('expert', 'shard'), may hold values from -0.25 to 0.25
- master_up: float32 [64, 2048, 1024], P('expert', 'shard'), may hold values from -0.25 to 0.25
- master_down: float32 [64, 1024, 2048], P('expert', None, 'shard'), may hold values from -0.375 to 0.375
- router_weight: float32 [2048, 64], P('shard', 'expert'), may hold values from -0.125 to 0.125
- router_gain: float32 [2048], P('shard'), may hold values from 0.25 to 1.75
Outputs:
- final_gate: bfloat16 [64, 2048, 1024], P('expert', None, 'shard')
- final_up: bfloat16 [64, 2048, 1024], P('expert', None, 'shard')
- final_down: bfloat16 [64, 1024, 2048], P('expert', 'shard')
- scale_gate: float32 [64, 1024], P('expert', 'shard')
- scale_up: float32 [64, 1024], P('expert', 'shard')
- scale_down: float32 [64, 1024], P('expert', 'shard')
- serve_router: bfloat16 [2048, 64], replicated
The draws below stay inside these ranges and needn't reach their ends.
All inputs are finite; a program needn't handle non-finite values.
Results may differ from the reference program's by a relative error of at most 0.001.
Values may be sent and summed in bfloat16 or wider, within the bound.
A program may use at most 128 MiB of HBM per device.

```python
import jax
import jax.numpy as jnp
from jax import lax

EXPERTS = 64
D_MODEL = 2048
D_EXPERT = 1024


def with_spikes(entries, rng, source, target, shards_of, factor):
    def block_of(axis_at):
        return (jnp.arange(entries.shape[axis_at]) // (entries.shape[axis_at] // shards_of)).reshape((-1,) + (1,) * (entries.ndim - 1 - axis_at))

    first = jax.random.permutation(rng, shards_of)[block_of(target)]
    far = (block_of(target) + shards_of // 2) % shards_of
    return jnp.where((block_of(source) == first) | (block_of(source) == far), factor * entries, entries)


def levels(stream_key, dims, split, smallest, high):
    factor_of = 1.0
    for position, parts in split:
        steps = jax.random.uniform(jax.random.fold_in(jax.random.fold_in(stream_key, 6), position), (parts,), jnp.float32, smallest / len(split), high / len(split))
        factor_of = factor_of * jnp.repeat(jnp.exp(steps), dims[position] // parts).reshape((-1,) + (1,) * (len(dims) - 1 - position))
    return factor_of


def centred(stream_key, extent, width, bound, split=(), held_as=jnp.bfloat16):
    entries = width * jax.random.normal(stream_key, extent, jnp.float32)
    if split:
        entries = entries * levels(stream_key, extent, split, -0.22, 0.18)
    return jnp.clip(entries, -bound, bound).astype(held_as)


def bell_draw_with(rng, dims, spread, reach, pieces, heavy, dtype=jnp.bfloat16):
    values = spread * jax.random.normal(rng, dims, jnp.float32)
    if pieces:
        values = values * levels(rng, dims, pieces, -0.22, 0.18)
    return jnp.clip(with_spikes(values, jax.random.fold_in(rng, 3), *heavy), -reach, reach).astype(dtype)


def setup_inputs(seed: int = 0) -> dict:
    streams_of = jax.random.split(jax.random.key(seed), 6)
    return {
        "master_gate": bell_draw_with(streams_of[0], (EXPERTS, D_MODEL, D_EXPERT), D_MODEL ** -0.5, 0.25, ((0, 4), (1, 32)), (1, 2, 32, 2.75), jnp.float32),
        "master_up": bell_draw_with(streams_of[1], (EXPERTS, D_MODEL, D_EXPERT), D_MODEL ** -0.5, 0.25, ((0, 4), (1, 32)), (1, 2, 32, 2.75), jnp.float32),
        "master_down": bell_draw_with(streams_of[2], (EXPERTS, D_EXPERT, D_MODEL), D_EXPERT ** -0.5, 0.375, ((0, 4), (2, 32)), (2, 1, 32, 2.75), jnp.float32),
        "router_weight": centred(streams_of[3], (D_MODEL, EXPERTS), D_MODEL ** -0.5, 0.125, ((0, 32), (1, 4)), jnp.float32),
        "router_gain": jnp.clip(1.0 + 0.15 * jax.random.normal(streams_of[4], (D_MODEL,), jnp.float32), 0.25, 1.75),
    }


def reference(master_gate, master_up, master_down, router_weight, router_gain):
    scale_gate = jnp.sqrt(lax.optimization_barrier(jnp.sum(master_gate * master_gate, axis=1)))
    final_gate = (master_gate / jnp.expand_dims(scale_gate, 1)).astype(jnp.bfloat16)
    scale_up = jnp.sqrt(lax.optimization_barrier(jnp.sum(master_up * master_up, axis=1)))
    final_up = (master_up / jnp.expand_dims(scale_up, 1)).astype(jnp.bfloat16)
    scale_down = jnp.sqrt(lax.optimization_barrier(jnp.sum(master_down * master_down, axis=2)))
    final_down = (master_down / jnp.expand_dims(scale_down, 2)).astype(jnp.bfloat16)
    serve_router = (router_weight * router_gain[:, None]).astype(jnp.bfloat16)
    return (final_gate, final_up, final_down, scale_gate, scale_up, scale_down, serve_router)
```

```python
import functools

import jax
import jax.numpy as jnp
from jax import lax
from jax.experimental import pallas as pl
from jax.experimental.pallas import tpu as pltpu
from jax.sharding import Mesh
from jax.sharding import PartitionSpec as P

SHARD = ("shard_0", "shard_1", "shard_2")
EXPERT = ("expert_0", "expert_1")
MESH = pl.DeviceIdType.MESH

ORDER = tuple(
    ((k * 11) % 32 // 8, (k * 11) % 8 // 2, (k * 11) % 2) for k in range(1, 32)
)
PAIRS = 8
CUT = 8
CHUNKS = 3 * PAIRS // CUT


def place():
    xl, core, z, y, xh = (lax.axis_index(a) for a in EXPERT + SHARD)
    return xl, core, z, y, xh


def peer(where, offset):
    xl, core, z, y, xh = where
    dz, dy, dx = offset
    turn = 1 - 2 * core
    pz, py, px = (z + turn * dz + 4) % 4, (y + turn * dy + 4) % 4, (xh + dx) % 2
    return (xl, core, pz, py, px), (pz * 4 + py) * 2 + px


def exchange(
    gate, up, down, router, gain,
    landed, routed, scales,
    rows, part, parts, scale, ready, mine,
    load_sem, sum_send, sum_recv, all_send, all_recv,
    data_send, data_recv, own_sem, r_send, r_recv, g_send, g_recv, r_own,
):
    where = place()
    xl, core, z, y, xh = where
    block = z * 4 + y
    me = block * 2 + xh
    group = xl * 2 + core
    peers = [peer(where, offset) for offset in ORDER]
    planes = [(xl, core, (z + dz) % 4, (y + dy) % 4, xh) for dz in range(4) for dy in range(4) if dz or dy]
    twins = ((xl, 1 - core, z, y, xh), (1 - xl, core, z, y, xh))

    loads = [
        pltpu.make_async_copy(source, rows.at[t], load_sem.at[t])
        for t, source in enumerate((gate, up, down))
    ]
    for load in loads:
        load.start()
    barrier = pltpu.get_barrier_semaphore()
    for device, _ in peers:
        pl.semaphore_signal(barrier, inc=1, device_id=device, device_id_type=MESH)
    for device in twins:
        pl.semaphore_signal(barrier, inc=1, device_id=device, device_id_type=MESH)

    narrow = (router[...] * gain[...]).astype(jnp.bfloat16).astype(jnp.float32)
    mine[...] = jnp.concatenate([narrow[0:8], narrow[8:16]], axis=1).astype(jnp.bfloat16)

    for t in range(3):
        loads[t].wait()

        def add_up(e, carry):
            for k in range(8):
                value = rows[t, e, :, pl.ds(k * 128, 128)]
                part[t, e, pl.ds(k, 1), :] = jnp.sum(value * value, axis=0, keepdims=True)
            return carry

        lax.fori_loop(0, 16, add_up, 0)
        if t == 0:
            pl.semaphore_wait(barrier, 33)
        for k, (device, index) in enumerate(peers):
            pltpu.make_async_remote_copy(
                part.at[t, index // 2], parts.at[t, me], sum_send.at[t], sum_recv.at[t],
                device_id=device, device_id_type=MESH,
            ).start()
        parts[t, me] = part[t, block]
        if t == 0:
            for device, _ in peers:
                pltpu.make_async_remote_copy(
                    mine, routed.at[group, me], r_send, r_recv, device_id=device, device_id_type=MESH
                ).start()
            own = pltpu.make_async_copy(mine, routed.at[group, me], r_own)
            own.start()
            own.wait()

    for t in range(3):
        pltpu.make_async_copy(parts.at[t, pl.ds(0, 31)], parts.at[t, pl.ds(0, 31)], sum_recv.at[t]).wait()
        total = parts[t, 0]
        for s in range(1, 32):
            total = total + parts[t, s]
        scale[t, block] = jnp.sqrt(total)
        for device in planes:
            pltpu.make_async_remote_copy(
                scale.at[t, block], scale.at[t, block], all_send.at[t], all_recv.at[t],
                device_id=device, device_id_type=MESH,
            ).start()

    for t in range(3):
        pltpu.make_async_copy(scale.at[t, pl.ds(0, 15)], scale.at[t, pl.ds(0, 15)], all_recv.at[t]).wait()

        def narrowed(p, carry):
            q = t * (PAIRS // CUT) + p // CUT
            for k in range(8):
                low = rows[t, 2 * p, :, pl.ds(k * 128, 128)] * (1.0 / scale[t, 2 * p, pl.ds(k, 1), :])
                high = rows[t, 2 * p + 1, :, pl.ds(k * 128, 128)] * (1.0 / scale[t, 2 * p + 1, pl.ds(k, 1), :])
                both = jnp.concatenate([low, high], axis=0)
                ready[q, pl.ds(4 * k, 4), p % CUT] = both.T.astype(jnp.bfloat16).reshape(4, 32, 128)
            return carry

        for part_of in range(PAIRS // CUT):
            q = t * (PAIRS // CUT) + part_of
            lax.fori_loop(part_of * CUT, part_of * CUT + CUT, narrowed, 0)
            for device, index in peers:
                pltpu.make_async_remote_copy(
                    ready.at[q, index], landed.at[q, me], data_send.at[q], data_recv.at[q],
                    device_id=device, device_id_type=MESH,
                ).start()
            pltpu.make_async_copy(ready.at[q, me], landed.at[q, me], own_sem.at[q]).start()
        rolled = pltpu.roll(scale[t, :, me // 4, :], (128 - 32 * (me % 4)) % 128, 1)
        scales[t] = rolled[:, 0:32]
        if t == 0:
            pltpu.make_async_copy(routed.at[group, pl.ds(0, 31)], routed.at[group, pl.ds(0, 31)], r_recv).wait()
            for k, device in enumerate(twins):
                pltpu.make_async_remote_copy(
                    routed.at[group], routed.at[group], g_send.at[k], g_recv.at[k], device_id=device, device_id_type=MESH
                ).start()
        if t == 1:
            pltpu.make_async_copy(routed.at[0], routed.at[0], g_recv.at[1]).wait()
            other = (1 - xl) * 2 + core
            pltpu.make_async_remote_copy(
                routed.at[other], routed.at[other], g_send.at[2], g_recv.at[2], device_id=twins[0], device_id_type=MESH
            ).start()

    for k in (0, 2):
        pltpu.make_async_copy(routed.at[0], routed.at[0], g_recv.at[k]).wait()
    for k in range(3):
        pltpu.make_async_copy(routed.at[0], routed.at[0], g_send.at[k]).wait()
    pltpu.make_async_copy(routed.at[0, pl.ds(0, 31)], routed.at[0, pl.ds(0, 31)], r_send).wait()
    for t in range(3):
        pltpu.make_async_copy(parts.at[t, pl.ds(0, 31)], parts.at[t, pl.ds(0, 31)], sum_send.at[t]).wait()
        pltpu.make_async_copy(scale.at[t, pl.ds(0, 15)], scale.at[t, pl.ds(0, 15)], all_send.at[t]).wait()
    for q in range(CHUNKS):
        pltpu.make_async_copy(ready.at[q, me], landed.at[q, me], own_sem.at[q]).wait()
        pltpu.make_async_copy(ready.at[q, pl.ds(0, 31)], ready.at[q, pl.ds(0, 31)], data_send.at[q]).wait()
        pltpu.make_async_copy(ready.at[q, pl.ds(0, 31)], ready.at[q, pl.ds(0, 31)], data_recv.at[q]).wait()


def moved(gate, up, down, router, gain):
    hbm = pl.BlockSpec(memory_space=pl.ANY)
    vmem = pl.BlockSpec(memory_space=pltpu.VMEM)
    dma = pltpu.SemaphoreType.DMA
    return pl.pallas_call(
        exchange,
        name="exchange",
        out_shape=(
            jax.ShapeDtypeStruct((CHUNKS, 32, CUT, 32, 128), jnp.bfloat16),
            jax.ShapeDtypeStruct((4, 32, 8, 128), jnp.bfloat16),
            jax.ShapeDtypeStruct((3, 16, 32), jnp.float32),
        ),
        in_specs=[hbm, hbm, hbm, vmem, vmem],
        out_specs=(hbm, hbm, vmem),
        scratch_shapes=[
            pltpu.VMEM((3, 16, 64, 1024), jnp.float32),
            pltpu.VMEM((3, 16, 8, 128), jnp.float32),
            pltpu.VMEM((3, 32, 8, 128), jnp.float32),
            pltpu.VMEM((3, 16, 8, 128), jnp.float32),
            pltpu.VMEM((CHUNKS, 32, CUT, 32, 128), jnp.bfloat16),
            pltpu.VMEM((8, 128), jnp.bfloat16),
            dma((3,)), dma((3,)), dma((3,)), dma((3,)), dma((3,)),
            dma((CHUNKS,)), dma((CHUNKS,)), dma((CHUNKS,)),
            dma, dma, dma((3,)), dma((3,)), dma,
        ],
        compiler_params=pltpu.CompilerParams(collective_id=0, has_side_effects=True),
    )(gate, up, down, router, gain)


STEP = 4


def halves(first, second):
    low = jnp.concatenate([first[..., 0:64], second[..., 0:64]], axis=-1)
    high = jnp.concatenate([first[..., 64:128], second[..., 64:128]], axis=-1)
    return low, high


def settle(landed, routed, gate, up, down, router):
    t, step = pl.program_id(0), pl.program_id(1)

    @pl.when((t == 0) & (step == 0))
    def _():
        for g in range(4):
            for k in range(16):
                low, high = halves(routed[g, 2 * k], routed[g, 2 * k + 1])
                router[pl.ds(16 * g, 8), pl.ds(k * 128, 128)] = low
                router[pl.ds(16 * g + 8, 8), pl.ds(k * 128, 128)] = high

    for at, out in enumerate((gate, up, down)):

        @pl.when(t == at)
        def _():
            def put(p, carry):
                for k in range(16):
                    low, high = halves(landed[0, 2 * k, p], landed[0, 2 * k + 1, p])
                    out[2 * p, :, pl.ds(k * 128, 128)] = low
                    out[2 * p + 1, :, pl.ds(k * 128, 128)] = high
                return carry

            lax.fori_loop(0, STEP, put, 0)


def settled(landed, routed):
    steps, per = PAIRS // STEP, CUT // STEP

    def spot(at):
        return lambda t, s: (jnp.where(t == at, s, jnp.where(t < at, 0, steps - 1)), 0, 0)

    return pl.pallas_call(
        settle,
        name="settle",
        grid=(3, steps),
        out_shape=tuple(jax.ShapeDtypeStruct((16, 32, 2048), jnp.bfloat16) for _ in range(3))
        + (jax.ShapeDtypeStruct((64, 2048), jnp.bfloat16),),
        in_specs=[
            pl.BlockSpec(
                (1, 32, STEP, 32, 128),
                lambda t, s: (t * (PAIRS // CUT) + s // per, 0, s % per, 0, 0),
            ),
            pl.BlockSpec((4, 32, 8, 128), lambda t, s: (0, 0, 0, 0)),
        ],
        out_specs=tuple(pl.BlockSpec((2 * STEP, 32, 2048), spot(at)) for at in range(3))
        + (pl.BlockSpec((64, 2048), lambda t, s: (0, 0)),),
        compiler_params=pltpu.CompilerParams(dimension_semantics=("arbitrary", "arbitrary")),
    )(landed, routed)


def on_device(master_gate, master_up, master_down, router_weight, router_gain):
    landed, routed, scales = moved(
        master_gate, master_up, master_down.transpose(0, 2, 1), router_weight.T, router_gain.reshape(1, 64)
    )
    gate, up, down, router = settled(landed, routed)
    return (
        gate.transpose(0, 2, 1), up.transpose(0, 2, 1), down,
        scales[0], scales[1], scales[2], router.T,
    )


def solution(mesh):
    torus = Mesh(
        mesh.devices.reshape(2, 2, 4, 4, 2),
        ("expert_0", "expert_1", "shard_0", "shard_1", "shard_2"),
    )
    return jax.shard_map(
        on_device,
        mesh=torus,
        in_specs=(
            P(EXPERT, SHARD, None),
            P(EXPERT, SHARD, None),
            P(EXPERT, None, SHARD),
            P(SHARD, EXPERT),
            P(SHARD),
        ),
        out_specs=(
            P(EXPERT, None, SHARD),
            P(EXPERT, None, SHARD),
            P(EXPERT, SHARD, None),
            P(EXPERT, SHARD),
            P(EXPERT, SHARD),
            P(EXPERT, SHARD),
            P(),
        ),
        check_vma=False,
    )
```

```python
import functools

import jax
import jax.numpy as jnp
from jax import lax
from jax.experimental import pallas as pl
from jax.experimental.pallas import tpu as pltpu
from jax.sharding import Mesh
from jax.sharding import PartitionSpec as P

SHARD = ("shard_0", "shard_1", "shard_2")
EXPERT = ("expert_0", "expert_1")
MESH = pl.DeviceIdType.MESH

ORDER = tuple(
    ((k * 11) % 32 // 8, (k * 11) % 8 // 2, (k * 11) % 2) for k in range(1, 32)
)
PAIRS = 8
CUT = 4
CHUNKS = 3 * PAIRS // CUT


def place():
    xl, core, z, y, xh = (lax.axis_index(a) for a in EXPERT + SHARD)
    return xl, core, z, y, xh


def peer(where, offset):
    xl, core, z, y, xh = where
    dz, dy, dx = offset
    turn = 1 - 2 * core
    pz, py, px = (z + turn * dz + 4) % 4, (y + turn * dy + 4) % 4, (xh + dx) % 2
    return (xl, core, pz, py, px), (pz * 4 + py) * 2 + px


def halves(first, second):
    low = jnp.concatenate([first[..., 0:64], second[..., 0:64]], axis=-1)
    high = jnp.concatenate([first[..., 64:128], second[..., 64:128]], axis=-1)
    return low, high


def exchange(
    gate, up, down, router_at, gain_at,
    out_gate, out_up, out_down, out_router, scale_gate, scale_up, scale_down,
    landed, routed, router, gain, rows, part, parts, scale, ready, mine,
    load_sem, sum_send, sum_recv, all_send, all_recv,
    data_send, data_recv, own_sem, r_send, r_recv, g_send, g_recv, r_own,
):
    where = place()
    xl, core, z, y, xh = where
    block = z * 4 + y
    me = block * 2 + xh
    group = xl * 2 + core
    peers = [peer(where, offset) for offset in ORDER]
    planes = [(xl, core, (z + dz) % 4, (y + dy) % 4, xh) for dz in range(4) for dy in range(4) if dz or dy]
    twins = ((xl, 1 - core, z, y, xh), (1 - xl, core, z, y, xh))

    loads = [
        pltpu.make_async_copy(source, rows.at[t], load_sem.at[t])
        for t, source in enumerate((gate, up, down))
    ]
    for load in loads:
        load.start()
    smalls = [
        pltpu.make_async_copy(source, target, load_sem.at[3 + k])
        for k, (source, target) in enumerate(((router_at, router), (gain_at, gain)))
    ]
    for load in smalls:
        load.start()
    barrier = pltpu.get_barrier_semaphore()
    for device, _ in peers:
        pl.semaphore_signal(barrier, inc=1, device_id=device, device_id_type=MESH)
    for device in twins:
        pl.semaphore_signal(barrier, inc=1, device_id=device, device_id_type=MESH)

    for load in smalls:
        load.wait()
    narrow = (router[...] * gain[...]).astype(jnp.bfloat16).astype(jnp.float32)
    mine[...] = jnp.concatenate([narrow[0:8], narrow[8:16]], axis=1).astype(jnp.bfloat16)

    for t in range(3):
        loads[t].wait()

        def add_up(e, carry):
            for k in range(8):
                value = rows[t, e, :, pl.ds(k * 128, 128)]
                part[t, e, pl.ds(k, 1), :] = jnp.sum(value * value, axis=0, keepdims=True)
            return carry

        lax.fori_loop(0, 16, add_up, 0)
        if t == 0:
            pl.semaphore_wait(barrier, 33)
        for k, (device, index) in enumerate(peers):
            pltpu.make_async_remote_copy(
                part.at[t, index // 2], parts.at[t, me], sum_send.at[t], sum_recv.at[t],
                device_id=device, device_id_type=MESH,
            ).start()
        parts[t, me] = part[t, block]
        if t == 0:
            for device, _ in peers:
                pltpu.make_async_remote_copy(
                    mine, routed.at[group, me], r_send, r_recv, device_id=device, device_id_type=MESH
                ).start()
            own = pltpu.make_async_copy(mine, routed.at[group, me], r_own)
            own.start()
            own.wait()

    for t in range(3):
        pltpu.make_async_copy(parts.at[t, pl.ds(0, 31)], parts.at[t, pl.ds(0, 31)], sum_recv.at[t]).wait()
        total = parts[t, 0]
        for s in range(1, 32):
            total = total + parts[t, s]
        scale[t, block] = jnp.sqrt(total)
        for device in planes:
            pltpu.make_async_remote_copy(
                scale.at[t, block], scale.at[t, block], all_send.at[t], all_recv.at[t],
                device_id=device, device_id_type=MESH,
            ).start()

    for t in range(3):
        pltpu.make_async_copy(scale.at[t, pl.ds(0, 15)], scale.at[t, pl.ds(0, 15)], all_recv.at[t]).wait()

        def narrowed(p, carry):
            q = t * (PAIRS // CUT) + p // CUT
            for k in range(8):
                low = rows[t, 2 * p, :, pl.ds(k * 128, 128)] * (1.0 / scale[t, 2 * p, pl.ds(k, 1), :])
                high = rows[t, 2 * p + 1, :, pl.ds(k * 128, 128)] * (1.0 / scale[t, 2 * p + 1, pl.ds(k, 1), :])
                both = jnp.concatenate([low, high], axis=0)
                ready[q, pl.ds(4 * k, 4), p % CUT] = both.T.astype(jnp.bfloat16).reshape(4, 32, 128)
            return carry

        for part_of in range(PAIRS // CUT):
            q = t * (PAIRS // CUT) + part_of
            lax.fori_loop(part_of * CUT, part_of * CUT + CUT, narrowed, 0)
            for device, index in peers:
                pltpu.make_async_remote_copy(
                    ready.at[q, index], landed.at[q, me], data_send.at[q], data_recv.at[q],
                    device_id=device, device_id_type=MESH,
                ).start()
            pltpu.make_async_copy(ready.at[q, me], landed.at[q, me], own_sem.at[q]).start()
        rolled = pltpu.roll(scale[t, :, me // 4, :], (128 - 32 * (me % 4)) % 128, 1)
        (scale_gate, scale_up, scale_down)[t][...] = rolled[:, 0:32]
        if t == 0:
            pltpu.make_async_copy(routed.at[group, pl.ds(0, 31)], routed.at[group, pl.ds(0, 31)], r_recv).wait()
            for k, device in enumerate(twins):
                pltpu.make_async_remote_copy(
                    routed.at[group], routed.at[group], g_send.at[k], g_recv.at[k], device_id=device, device_id_type=MESH
                ).start()
        if t == 1:
            pltpu.make_async_copy(routed.at[0], routed.at[0], g_recv.at[1]).wait()
            other = (1 - xl) * 2 + core
            pltpu.make_async_remote_copy(
                routed.at[other], routed.at[other], g_send.at[2], g_recv.at[2], device_id=twins[0], device_id_type=MESH
            ).start()

    for t, out in enumerate((out_gate, out_up, out_down)):
        for part_of in range(PAIRS // CUT):
            q = t * (PAIRS // CUT) + part_of
            pltpu.make_async_copy(ready.at[q, me], landed.at[q, me], own_sem.at[q]).wait()
            pltpu.make_async_copy(ready.at[q, pl.ds(0, 31)], ready.at[q, pl.ds(0, 31)], data_recv.at[q]).wait()

            def put(p, carry):
                for k in range(16):
                    low, high = halves(landed[q, 2 * k, p], landed[q, 2 * k + 1, p])
                    expert = 2 * (part_of * CUT + p)
                    out[expert, :, pl.ds(k * 128, 128)] = low
                    out[expert + 1, :, pl.ds(k * 128, 128)] = high
                return carry

            lax.fori_loop(0, CUT, put, 0)
        if t == 1:
            for k in (0, 2):
                pltpu.make_async_copy(routed.at[0], routed.at[0], g_recv.at[k]).wait()

            def put_router(g, carry):
                for k in range(16):
                    low, high = halves(routed[g, 2 * k], routed[g, 2 * k + 1])
                    out_router[pl.ds(pl.multiple_of(16 * g, 16), 16), pl.ds(k * 128, 128)] = jnp.concatenate([low, high], axis=0)
                return carry

            lax.fori_loop(0, 4, put_router, 0)

    for k in range(3):
        pltpu.make_async_copy(routed.at[0], routed.at[0], g_send.at[k]).wait()
    pltpu.make_async_copy(routed.at[0, pl.ds(0, 31)], routed.at[0, pl.ds(0, 31)], r_send).wait()
    for t in range(3):
        pltpu.make_async_copy(parts.at[t, pl.ds(0, 31)], parts.at[t, pl.ds(0, 31)], sum_send.at[t]).wait()
        pltpu.make_async_copy(scale.at[t, pl.ds(0, 15)], scale.at[t, pl.ds(0, 15)], all_send.at[t]).wait()
    for q in range(CHUNKS):
        pltpu.make_async_copy(ready.at[q, pl.ds(0, 31)], ready.at[q, pl.ds(0, 31)], data_send.at[q]).wait()


def moved(gate, up, down, router, gain):
    hbm = pl.BlockSpec(memory_space=pl.ANY)
    vmem = pl.BlockSpec(memory_space=pltpu.VMEM)
    dma = pltpu.SemaphoreType.DMA
    return pl.pallas_call(
        exchange,
        name="exchange",
        out_shape=tuple(pltpu.VMEM((16, 32, 2048), jnp.bfloat16) for _ in range(3))
        + (pltpu.VMEM((64, 2048), jnp.bfloat16),)
        + tuple(pltpu.VMEM((16, 32), jnp.float32) for _ in range(3)),
        in_specs=[hbm] * 5,
        out_specs=(vmem,) * 7,
        scratch_shapes=[
            pltpu.VMEM((CHUNKS, 32, CUT, 32, 128), jnp.bfloat16),
            pltpu.VMEM((4, 32, 8, 128), jnp.bfloat16),
            pltpu.VMEM((16, 64), jnp.float32),
            pltpu.VMEM((1, 64), jnp.float32),
            pltpu.VMEM((3, 16, 64, 1024), jnp.float32),
            pltpu.VMEM((3, 16, 8, 128), jnp.float32),
            pltpu.VMEM((3, 32, 8, 128), jnp.float32),
            pltpu.VMEM((3, 16, 8, 128), jnp.float32),
            pltpu.VMEM((CHUNKS, 32, CUT, 32, 128), jnp.bfloat16),
            pltpu.VMEM((8, 128), jnp.bfloat16),
            dma((5,)), dma((3,)), dma((3,)), dma((3,)), dma((3,)),
            dma((CHUNKS,)), dma((CHUNKS,)), dma((CHUNKS,)),
            dma, dma, dma((3,)), dma((3,)), dma,
        ],
        compiler_params=pltpu.CompilerParams(collective_id=0, has_side_effects=True, vmem_limit_bytes=54 * 2**20),
    )(gate, up, down, router, gain)


def write_out(*refs):
    sources, targets, sem = refs[:7], refs[7:14], refs[14]
    copies = [pltpu.make_async_copy(sources[k], targets[k], sem.at[k]) for k in range(7)]
    for copy in copies:
        copy.start()
    for copy in copies:
        copy.wait()


def written(arrays):
    hbm = pl.BlockSpec(memory_space=pltpu.HBM)
    vmem = pl.BlockSpec(memory_space=pltpu.VMEM)
    return pl.pallas_call(
        write_out,
        name="write_out",
        out_shape=tuple(jax.ShapeDtypeStruct(v.shape, v.dtype) for v in arrays),
        in_specs=[vmem] * 7,
        out_specs=(hbm,) * 7,
        scratch_shapes=[pltpu.SemaphoreType.DMA((7,))],
        compiler_params=pltpu.CompilerParams(vmem_limit_bytes=2**20),
    )(*(pltpu.with_memory_space_constraint(v, pltpu.VMEM) for v in arrays))


def on_device(master_gate, master_up, master_down, router_weight, router_gain):
    held = (master_gate, master_up, master_down.transpose(0, 2, 1), router_weight.T, router_gain.reshape(1, 64))
    moved_arrays = moved(*(pltpu.with_memory_space_constraint(v, pltpu.HBM) for v in held))
    gate, up, down, router, *scales = written(moved_arrays)
    return (gate.transpose(0, 2, 1), up.transpose(0, 2, 1), down, *scales, router.T)


def solution(mesh):
    torus = Mesh(
        mesh.devices.reshape(2, 2, 4, 4, 2),
        ("expert_0", "expert_1", "shard_0", "shard_1", "shard_2"),
    )
    return jax.shard_map(
        on_device,
        mesh=torus,
        in_specs=(
            P(EXPERT, SHARD, None),
            P(EXPERT, SHARD, None),
            P(EXPERT, None, SHARD),
            P(SHARD, EXPERT),
            P(SHARD),
        ),
        out_specs=(
            P(EXPERT, None, SHARD),
            P(EXPERT, None, SHARD),
            P(EXPERT, SHARD, None),
            P(EXPERT, SHARD),
            P(EXPERT, SHARD),
            P(EXPERT, SHARD),
            P(),
        ),
        check_vma=False,
    )
```

```python
import functools

import jax
import jax.numpy as jnp
from jax import lax
from jax.experimental import pallas as pl
from jax.experimental.pallas import tpu as pltpu
from jax.sharding import Mesh
from jax.sharding import PartitionSpec as P

SHARD = ("shard_0", "shard_1", "shard_2")
EXPERT = ("expert_0", "expert_1")
MESH = pl.DeviceIdType.MESH

ORDER = tuple(
    (a, (a + step) % 4, (a + half) % 2)
    for step in range(4) for half in range(2) for a in range(4)
    if (a, (a + step) % 4, (a + half) % 2) != (0, 0, 0)
)
PAIRS = 8
CUT = 2
CHUNKS = 3 * PAIRS // CUT


def place():
    xl, core, z, y, xh = (lax.axis_index(a) for a in EXPERT + SHARD)
    return xl, core, z, y, xh


def peer(where, offset):
    xl, core, z, y, xh = where
    dz, dy, dx = offset
    turn = 1 - 2 * core
    pz, py, px = (z + turn * dz + 4) % 4, (y + turn * dy + 4) % 4, (xh + dx) % 2
    return (xl, core, pz, py, px), (pz * 4 + py) * 2 + px


def halves(first, second):
    low = jnp.concatenate([first[..., 0:64], second[..., 0:64]], axis=-1)
    high = jnp.concatenate([first[..., 64:128], second[..., 64:128]], axis=-1)
    return low, high


def exchange(
    gate, up, down, router_at, gain_at,
    out_gate, out_up, out_down, out_router, scale_gate, scale_up, scale_down,
    landed, routed, router, gain, rows, part, parts, scale, ready, mine,
    load_sem, sum_send, sum_recv, all_send, all_recv,
    data_send, data_recv, own_sem, r_send, r_recv, g_send, g_recv, r_own,
):
    where = place()
    xl, core, z, y, xh = where
    block = z * 4 + y
    me = block * 2 + xh
    group = xl * 2 + core
    peers = [peer(where, offset) for offset in ORDER]
    planes = [(xl, core, (z + dz) % 4, (y + dy) % 4, xh) for dz in range(4) for dy in range(4) if dz or dy]
    twins = ((xl, 1 - core, z, y, xh), (1 - xl, core, z, y, xh), (1 - xl, core, z, y, 1 - xh))

    loads = [
        pltpu.make_async_copy(source, rows.at[t], load_sem.at[t])
        for t, source in enumerate((gate, up, down))
    ]
    loads[0].start()
    smalls = [
        pltpu.make_async_copy(source, target, load_sem.at[3 + k])
        for k, (source, target) in enumerate(((router_at, router), (gain_at, gain)))
    ]
    for load in smalls:
        load.start()
    barrier = pltpu.get_barrier_semaphore()
    for device, _ in peers:
        pl.semaphore_signal(barrier, inc=1, device_id=device, device_id_type=MESH)
    for device in twins:
        pl.semaphore_signal(barrier, inc=1, device_id=device, device_id_type=MESH)

    for load in smalls:
        load.wait()
    narrow = (router[...] * gain[...]).astype(jnp.bfloat16).astype(jnp.float32)
    mine[...] = jnp.concatenate([narrow[0:8], narrow[8:16]], axis=1).astype(jnp.bfloat16)

    for t in range(3):
        loads[t].wait()
        if t < 2:
            loads[t + 1].start()

        def add_up(e, carry):
            for k in range(8):
                value = rows[t, e, :, pl.ds(k * 128, 128)]
                part[t, e, pl.ds(k, 1), :] = jnp.sum(value * value, axis=0, keepdims=True)
            return carry

        lax.fori_loop(0, 16, add_up, 0)
        if t == 0:
            pl.semaphore_wait(barrier, 34)
        for k, (device, index) in enumerate(peers):
            pltpu.make_async_remote_copy(
                part.at[t, index // 2], parts.at[t, me], sum_send.at[t], sum_recv.at[t],
                device_id=device, device_id_type=MESH,
            ).start()
        parts[t, me] = part[t, block]
        if t == 0:
            for device, _ in peers:
                pltpu.make_async_remote_copy(
                    mine, routed.at[group, me], r_send, r_recv, device_id=device, device_id_type=MESH
                ).start()
            own = pltpu.make_async_copy(mine, routed.at[group, me], r_own)
            own.start()
            own.wait()

    for t in range(3):
        pltpu.make_async_copy(parts.at[t, pl.ds(0, 31)], parts.at[t, pl.ds(0, 31)], sum_recv.at[t]).wait()
        total = parts[t, 0]
        for s in range(1, 32):
            total = total + parts[t, s]
        scale[t, block] = jnp.sqrt(total)
        for device in planes:
            pltpu.make_async_remote_copy(
                scale.at[t, block], scale.at[t, block], all_send.at[t], all_recv.at[t],
                device_id=device, device_id_type=MESH,
            ).start()

    for t in range(3):
        pltpu.make_async_copy(scale.at[t, pl.ds(0, 15)], scale.at[t, pl.ds(0, 15)], all_recv.at[t]).wait()

        def narrowed(p, carry):
            q = t * (PAIRS // CUT) + p // CUT
            for k in range(8):
                low = rows[t, 2 * p, :, pl.ds(k * 128, 128)] * (1.0 / scale[t, 2 * p, pl.ds(k, 1), :])
                high = rows[t, 2 * p + 1, :, pl.ds(k * 128, 128)] * (1.0 / scale[t, 2 * p + 1, pl.ds(k, 1), :])
                both = jnp.concatenate([low, high], axis=0)
                ready[q, pl.ds(4 * k, 4), p % CUT] = both.T.astype(jnp.bfloat16).reshape(4, 32, 128)
            return carry

        for part_of in range(PAIRS // CUT):
            q = t * (PAIRS // CUT) + part_of
            lax.fori_loop(part_of * CUT, part_of * CUT + CUT, narrowed, 0)
            first = q * 5 % 31
            for device, index in peers[first:] + peers[:first]:
                pltpu.make_async_remote_copy(
                    ready.at[q, index], landed.at[q, me], data_send.at[q], data_recv.at[q],
                    device_id=device, device_id_type=MESH,
                ).start()
            pltpu.make_async_copy(ready.at[q, me], landed.at[q, me], own_sem.at[q]).start()
        rolled = pltpu.roll(scale[t, :, me // 4, :], (128 - 32 * (me % 4)) % 128, 1)
        (scale_gate, scale_up, scale_down)[t][...] = rolled[:, 0:32]
        if t == 0:
            pltpu.make_async_copy(routed.at[group, pl.ds(0, 31)], routed.at[group, pl.ds(0, 31)], r_recv).wait()
            pltpu.make_async_remote_copy(
                routed.at[group], routed.at[group], g_send.at[0], g_recv.at[0], device_id=twins[0], device_id_type=MESH
            ).start()
            for k in range(2):
                half = routed.at[group, pl.ds(16 * k, 16)]
                pltpu.make_async_remote_copy(
                    half, half, g_send.at[1 + k], g_recv.at[1 + k], device_id=twins[1 + k], device_id_type=MESH
                ).start()
        if t == 1:
            for k in (1, 2):
                pltpu.make_async_copy(routed.at[0, pl.ds(0, 16)], routed.at[0, pl.ds(0, 16)], g_recv.at[k]).wait()
            other = (1 - xl) * 2 + core
            pltpu.make_async_remote_copy(
                routed.at[other], routed.at[other], g_send.at[3], g_recv.at[3], device_id=twins[0], device_id_type=MESH
            ).start()

    for t, out in enumerate((out_gate, out_up, out_down)):
        for part_of in range(PAIRS // CUT):
            q = t * (PAIRS // CUT) + part_of
            pltpu.make_async_copy(ready.at[q, me], landed.at[q, me], own_sem.at[q]).wait()
            pltpu.make_async_copy(ready.at[q, pl.ds(0, 31)], ready.at[q, pl.ds(0, 31)], data_recv.at[q]).wait()

            def put(p, carry):
                for k in range(16):
                    low, high = halves(landed[q, 2 * k, p], landed[q, 2 * k + 1, p])
                    expert = 2 * (part_of * CUT + p)
                    out[expert, :, pl.ds(k * 128, 128)] = low
                    out[expert + 1, :, pl.ds(k * 128, 128)] = high
                return carry

            lax.fori_loop(0, CUT, put, 0)
        if t == 1:
            for k in (0, 3):
                pltpu.make_async_copy(routed.at[0], routed.at[0], g_recv.at[k]).wait()

            def put_router(g, carry):
                for k in range(16):
                    low, high = halves(routed[g, 2 * k], routed[g, 2 * k + 1])
                    out_router[pl.ds(pl.multiple_of(16 * g, 16), 16), pl.ds(k * 128, 128)] = jnp.concatenate([low, high], axis=0)
                return carry

            lax.fori_loop(0, 4, put_router, 0)

    for k in (0, 3):
        pltpu.make_async_copy(routed.at[0], routed.at[0], g_send.at[k]).wait()
    for k in (1, 2):
        pltpu.make_async_copy(routed.at[0, pl.ds(0, 16)], routed.at[0, pl.ds(0, 16)], g_send.at[k]).wait()
    pltpu.make_async_copy(routed.at[0, pl.ds(0, 31)], routed.at[0, pl.ds(0, 31)], r_send).wait()
    for t in range(3):
        pltpu.make_async_copy(parts.at[t, pl.ds(0, 31)], parts.at[t, pl.ds(0, 31)], sum_send.at[t]).wait()
        pltpu.make_async_copy(scale.at[t, pl.ds(0, 15)], scale.at[t, pl.ds(0, 15)], all_send.at[t]).wait()
    for q in range(CHUNKS):
        pltpu.make_async_copy(ready.at[q, pl.ds(0, 31)], ready.at[q, pl.ds(0, 31)], data_send.at[q]).wait()


def moved(gate, up, down, router, gain):
    hbm = pl.BlockSpec(memory_space=pl.ANY)
    vmem = pl.BlockSpec(memory_space=pltpu.VMEM)
    dma = pltpu.SemaphoreType.DMA
    return pl.pallas_call(
        exchange,
        name="exchange",
        out_shape=tuple(pltpu.VMEM((16, 32, 2048), jnp.bfloat16) for _ in range(3))
        + (pltpu.VMEM((64, 2048), jnp.bfloat16),)
        + tuple(pltpu.VMEM((16, 32), jnp.float32) for _ in range(3)),
        in_specs=[hbm] * 5,
        out_specs=(vmem,) * 7,
        scratch_shapes=[
            pltpu.VMEM((CHUNKS, 32, CUT, 32, 128), jnp.bfloat16),
            pltpu.VMEM((4, 32, 8, 128), jnp.bfloat16),
            pltpu.VMEM((16, 64), jnp.float32),
            pltpu.VMEM((1, 64), jnp.float32),
            pltpu.VMEM((3, 16, 64, 1024), jnp.float32),
            pltpu.VMEM((3, 16, 8, 128), jnp.float32),
            pltpu.VMEM((3, 32, 8, 128), jnp.float32),
            pltpu.VMEM((3, 16, 8, 128), jnp.float32),
            pltpu.VMEM((CHUNKS, 32, CUT, 32, 128), jnp.bfloat16),
            pltpu.VMEM((8, 128), jnp.bfloat16),
            dma((5,)), dma((3,)), dma((3,)), dma((3,)), dma((3,)),
            dma((CHUNKS,)), dma((CHUNKS,)), dma((CHUNKS,)),
            dma, dma, dma((4,)), dma((4,)), dma,
        ],
        compiler_params=pltpu.CompilerParams(collective_id=0, has_side_effects=True, vmem_limit_bytes=54 * 2**20),
    )(gate, up, down, router, gain)


def write_out(*refs):
    sources, targets, sem = refs[:7], refs[7:14], refs[14]
    copies = [pltpu.make_async_copy(sources[k], targets[k], sem.at[k]) for k in range(7)]
    for copy in copies:
        copy.start()
    for copy in copies:
        copy.wait()


def written(arrays):
    hbm = pl.BlockSpec(memory_space=pltpu.HBM)
    vmem = pl.BlockSpec(memory_space=pltpu.VMEM)
    return pl.pallas_call(
        write_out,
        name="write_out",
        out_shape=tuple(jax.ShapeDtypeStruct(v.shape, v.dtype) for v in arrays),
        in_specs=[vmem] * 7,
        out_specs=(hbm,) * 7,
        scratch_shapes=[pltpu.SemaphoreType.DMA((7,))],
        compiler_params=pltpu.CompilerParams(vmem_limit_bytes=2**20),
    )(*(pltpu.with_memory_space_constraint(v, pltpu.VMEM) for v in arrays))


def on_device(master_gate, master_up, master_down, router_weight, router_gain):
    held = (master_gate, master_up, master_down.transpose(0, 2, 1), router_weight.T, router_gain.reshape(1, 64))
    moved_arrays = moved(*(pltpu.with_memory_space_constraint(v, pltpu.HBM) for v in held))
    gate, up, down, router, *scales = written(moved_arrays)
    return (gate.transpose(0, 2, 1), up.transpose(0, 2, 1), down, *scales, router.T)


def solution(mesh):
    torus = Mesh(
        mesh.devices.reshape(2, 2, 4, 4, 2),
        ("expert_0", "expert_1", "shard_0", "shard_1", "shard_2"),
    )
    return jax.shard_map(
        on_device,
        mesh=torus,
        in_specs=(
            P(EXPERT, SHARD, None),
            P(EXPERT, SHARD, None),
            P(EXPERT, None, SHARD),
            P(SHARD, EXPERT),
            P(SHARD),
        ),
        out_specs=(
            P(EXPERT, None, SHARD),
            P(EXPERT, None, SHARD),
            P(EXPERT, SHARD, None),
            P(EXPERT, SHARD),
            P(EXPERT, SHARD),
            P(EXPERT, SHARD),
            P(),
        ),
        check_vma=False,
    )
```

```python
import functools

import jax
import jax.numpy as jnp
from jax import lax
from jax.experimental import pallas as pl
from jax.experimental.pallas import tpu as pltpu
from jax.sharding import Mesh
from jax.sharding import PartitionSpec as P

SHARD = ("shard_0", "shard_1", "shard_2")
EXPERT = ("expert_0", "expert_1")
MESH = pl.DeviceIdType.MESH

ORDER = tuple(
    (a, (a + step) % 4, (a + half) % 2)
    for step in range(4) for half in range(2) for a in range(4)
    if (a, (a + step) % 4, (a + half) % 2) != (0, 0, 0)
)
FAR_FIRST = sorted(range(31), key=lambda k: -sum((0, 1, 2, 1)[v] for v in ORDER[k][:2]) - 2 * ORDER[k][2])
PAIRS = 8
CUT = 2
LAST = 4
CHUNKS = 3 * PAIRS // CUT


def place():
    xl, core, z, y, xh = (lax.axis_index(a) for a in EXPERT + SHARD)
    return xl, core, z, y, xh


def peer(where, offset):
    xl, core, z, y, xh = where
    dz, dy, dx = offset
    turn = 1 - 2 * core
    pz, py, px = (z + turn * dz + 4) % 4, (y + turn * dy + 4) % 4, (xh + dx) % 2
    return (xl, core, pz, py, px), (pz * 4 + py) * 2 + px


def halves(first, second):
    low = jnp.concatenate([first[..., 0:64], second[..., 0:64]], axis=-1)
    high = jnp.concatenate([first[..., 64:128], second[..., 64:128]], axis=-1)
    return low, high


def exchange(
    gate, up, down, router_at, gain_at,
    out_gate, out_up, out_down, out_router, scale_gate, scale_up, scale_down,
    landed, routed, router, gain, rows, part, parts, scale, ready, mine,
    load_sem, sum_send, sum_recv, all_send, all_recv,
    data_send, data_recv, own_sem, r_send, r_recv, g_send, g_recv, r_own,
):
    where = place()
    xl, core, z, y, xh = where
    block = z * 4 + y
    me = block * 2 + xh
    group = xl * 2 + core
    peers = [peer(where, offset) for offset in ORDER]
    planes = [(xl, core, (z + dz) % 4, (y + dy) % 4, xh) for dz in range(4) for dy in range(4) if dz or dy]
    twins = ((xl, 1 - core, z, y, xh), (1 - xl, core, z, y, xh), (1 - xl, core, z, y, 1 - xh))

    loads = [
        pltpu.make_async_copy(source, rows.at[t], load_sem.at[t])
        for t, source in enumerate((gate, up, down))
    ]
    loads[0].start()
    smalls = [
        pltpu.make_async_copy(source, target, load_sem.at[3 + k])
        for k, (source, target) in enumerate(((router_at, router), (gain_at, gain)))
    ]
    for load in smalls:
        load.start()
    barrier = pltpu.get_barrier_semaphore()
    for device, _ in peers:
        pl.semaphore_signal(barrier, inc=1, device_id=device, device_id_type=MESH)
    for device in twins:
        pl.semaphore_signal(barrier, inc=1, device_id=device, device_id_type=MESH)

    for load in smalls:
        load.wait()
    narrow = (router[...] * gain[...]).astype(jnp.bfloat16).astype(jnp.float32)
    mine[...] = jnp.concatenate([narrow[0:8], narrow[8:16]], axis=1).astype(jnp.bfloat16)

    for t in range(3):
        loads[t].wait()
        if t < 2:
            loads[t + 1].start()

        def add_up(e, carry):
            for k in range(8):
                value = rows[t, e, :, pl.ds(k * 128, 128)]
                part[t, e, pl.ds(k, 1), :] = jnp.sum(value * value, axis=0, keepdims=True)
            return carry

        lax.fori_loop(0, 16, add_up, 0)
        if t == 0:
            pl.semaphore_wait(barrier, 34)
        for k, (device, index) in enumerate(peers):
            pltpu.make_async_remote_copy(
                part.at[t, index // 2], parts.at[t, me], sum_send.at[t], sum_recv.at[t],
                device_id=device, device_id_type=MESH,
            ).start()
        parts[t, me] = part[t, block]
        if t == 0:
            for device, _ in peers:
                pltpu.make_async_remote_copy(
                    mine, routed.at[group, me], r_send, r_recv, device_id=device, device_id_type=MESH
                ).start()
            own = pltpu.make_async_copy(mine, routed.at[group, me], r_own)
            own.start()
            own.wait()

    for t in range(3):
        pltpu.make_async_copy(parts.at[t, pl.ds(0, 31)], parts.at[t, pl.ds(0, 31)], sum_recv.at[t]).wait()
        total = parts[t, 0]
        for s in range(1, 32):
            total = total + parts[t, s]
        scale[t, block] = jnp.sqrt(total)
        for device in planes:
            pltpu.make_async_remote_copy(
                scale.at[t, block], scale.at[t, block], all_send.at[t], all_recv.at[t],
                device_id=device, device_id_type=MESH,
            ).start()

    def turned_by(q):
        return [(q * 5 + k) % 31 for k in range(31)]

    def send_out(messages):
        for q, k in messages:
            device, index = peers[k]
            pltpu.make_async_remote_copy(
                ready.at[q, index], landed.at[q, me], data_send.at[q], data_recv.at[q],
                device_id=device, device_id_type=MESH,
            ).start()
        for q in sorted({q for q, _ in messages}):
            pltpu.make_async_copy(ready.at[q, me], landed.at[q, me], own_sem.at[q]).start()

    for t in range(3):
        pltpu.make_async_copy(scale.at[t, pl.ds(0, 15)], scale.at[t, pl.ds(0, 15)], all_recv.at[t]).wait()

        def narrowed(p, carry):
            q = t * (PAIRS // CUT) + p // CUT
            for k in range(8):
                low = rows[t, 2 * p, :, pl.ds(k * 128, 128)] * (1.0 / scale[t, 2 * p, pl.ds(k, 1), :])
                high = rows[t, 2 * p + 1, :, pl.ds(k * 128, 128)] * (1.0 / scale[t, 2 * p + 1, pl.ds(k, 1), :])
                both = jnp.concatenate([low, high], axis=0)
                ready[q, pl.ds(4 * k, 4), p % CUT] = both.T.astype(jnp.bfloat16).reshape(4, 32, 128)
            return carry

        for part_of in range(PAIRS // CUT):
            q = t * (PAIRS // CUT) + part_of
            lax.fori_loop(part_of * CUT, part_of * CUT + CUT, narrowed, 0)
            if q < CHUNKS - LAST:
                send_out([(q, k) for k in turned_by(q)])
            elif q == CHUNKS - 1:
                send_out([(r, k) for k in FAR_FIRST for r in range(CHUNKS - LAST, CHUNKS)])
        rolled = pltpu.roll(scale[t, :, me // 4, :], (128 - 32 * (me % 4)) % 128, 1)
        (scale_gate, scale_up, scale_down)[t][...] = rolled[:, 0:32]
        if t == 0:
            pltpu.make_async_copy(routed.at[group, pl.ds(0, 31)], routed.at[group, pl.ds(0, 31)], r_recv).wait()
            pltpu.make_async_remote_copy(
                routed.at[group], routed.at[group], g_send.at[0], g_recv.at[0], device_id=twins[0], device_id_type=MESH
            ).start()
            for k in range(2):
                half = routed.at[group, pl.ds(16 * k, 16)]
                pltpu.make_async_remote_copy(
                    half, half, g_send.at[1 + k], g_recv.at[1 + k], device_id=twins[1 + k], device_id_type=MESH
                ).start()
        if t == 1:
            for k in (1, 2):
                pltpu.make_async_copy(routed.at[0, pl.ds(0, 16)], routed.at[0, pl.ds(0, 16)], g_recv.at[k]).wait()
            other = (1 - xl) * 2 + core
            pltpu.make_async_remote_copy(
                routed.at[other], routed.at[other], g_send.at[3], g_recv.at[3], device_id=twins[0], device_id_type=MESH
            ).start()

    for t, out in enumerate((out_gate, out_up, out_down)):
        for part_of in range(PAIRS // CUT):
            q = t * (PAIRS // CUT) + part_of
            pltpu.make_async_copy(ready.at[q, me], landed.at[q, me], own_sem.at[q]).wait()
            pltpu.make_async_copy(ready.at[q, pl.ds(0, 31)], ready.at[q, pl.ds(0, 31)], data_recv.at[q]).wait()

            def put(p, carry):
                for k in range(16):
                    low, high = halves(landed[q, 2 * k, p], landed[q, 2 * k + 1, p])
                    expert = 2 * (part_of * CUT + p)
                    out[expert, :, pl.ds(k * 128, 128)] = low
                    out[expert + 1, :, pl.ds(k * 128, 128)] = high
                return carry

            lax.fori_loop(0, CUT, put, 0)
        if t == 1:
            for k in (0, 3):
                pltpu.make_async_copy(routed.at[0], routed.at[0], g_recv.at[k]).wait()

            def put_router(g, carry):
                for k in range(16):
                    low, high = halves(routed[g, 2 * k], routed[g, 2 * k + 1])
                    out_router[pl.ds(pl.multiple_of(16 * g, 16), 16), pl.ds(k * 128, 128)] = jnp.concatenate([low, high], axis=0)
                return carry

            lax.fori_loop(0, 4, put_router, 0)

    for k in (0, 3):
        pltpu.make_async_copy(routed.at[0], routed.at[0], g_send.at[k]).wait()
    for k in (1, 2):
        pltpu.make_async_copy(routed.at[0, pl.ds(0, 16)], routed.at[0, pl.ds(0, 16)], g_send.at[k]).wait()
    pltpu.make_async_copy(routed.at[0, pl.ds(0, 31)], routed.at[0, pl.ds(0, 31)], r_send).wait()
    for t in range(3):
        pltpu.make_async_copy(parts.at[t, pl.ds(0, 31)], parts.at[t, pl.ds(0, 31)], sum_send.at[t]).wait()
        pltpu.make_async_copy(scale.at[t, pl.ds(0, 15)], scale.at[t, pl.ds(0, 15)], all_send.at[t]).wait()
    for q in range(CHUNKS):
        pltpu.make_async_copy(ready.at[q, pl.ds(0, 31)], ready.at[q, pl.ds(0, 31)], data_send.at[q]).wait()


def moved(gate, up, down, router, gain):
    hbm = pl.BlockSpec(memory_space=pl.ANY)
    vmem = pl.BlockSpec(memory_space=pltpu.VMEM)
    dma = pltpu.SemaphoreType.DMA
    return pl.pallas_call(
        exchange,
        name="exchange",
        out_shape=tuple(pltpu.VMEM((16, 32, 2048), jnp.bfloat16) for _ in range(3))
        + (pltpu.VMEM((64, 2048), jnp.bfloat16),)
        + tuple(pltpu.VMEM((16, 32), jnp.float32) for _ in range(3)),
        in_specs=[hbm] * 5,
        out_specs=(vmem,) * 7,
        scratch_shapes=[
            pltpu.VMEM((CHUNKS, 32, CUT, 32, 128), jnp.bfloat16),
            pltpu.VMEM((4, 32, 8, 128), jnp.bfloat16),
            pltpu.VMEM((16, 64), jnp.float32),
            pltpu.VMEM((1, 64), jnp.float32),
            pltpu.VMEM((3, 16, 64, 1024), jnp.float32),
            pltpu.VMEM((3, 16, 8, 128), jnp.float32),
            pltpu.VMEM((3, 32, 8, 128), jnp.float32),
            pltpu.VMEM((3, 16, 8, 128), jnp.float32),
            pltpu.VMEM((CHUNKS, 32, CUT, 32, 128), jnp.bfloat16),
            pltpu.VMEM((8, 128), jnp.bfloat16),
            dma((5,)), dma((3,)), dma((3,)), dma((3,)), dma((3,)),
            dma((CHUNKS,)), dma((CHUNKS,)), dma((CHUNKS,)),
            dma, dma, dma((4,)), dma((4,)), dma,
        ],
        compiler_params=pltpu.CompilerParams(collective_id=0, has_side_effects=True, vmem_limit_bytes=54 * 2**20),
    )(gate, up, down, router, gain)


def write_out(*refs):
    sources, targets, sem = refs[:7], refs[7:14], refs[14]
    copies = [pltpu.make_async_copy(sources[k], targets[k], sem.at[k]) for k in range(7)]
    for copy in copies:
        copy.start()
    for copy in copies:
        copy.wait()


def written(arrays):
    hbm = pl.BlockSpec(memory_space=pltpu.HBM)
    vmem = pl.BlockSpec(memory_space=pltpu.VMEM)
    return pl.pallas_call(
        write_out,
        name="write_out",
        out_shape=tuple(jax.ShapeDtypeStruct(v.shape, v.dtype) for v in arrays),
        in_specs=[vmem] * 7,
        out_specs=(hbm,) * 7,
        scratch_shapes=[pltpu.SemaphoreType.DMA((7,))],
        compiler_params=pltpu.CompilerParams(vmem_limit_bytes=2**20),
    )(*(pltpu.with_memory_space_constraint(v, pltpu.VMEM) for v in arrays))


def on_device(master_gate, master_up, master_down, router_weight, router_gain):
    held = (master_gate, master_up, master_down.transpose(0, 2, 1), router_weight.T, router_gain.reshape(1, 64))
    moved_arrays = moved(*(pltpu.with_memory_space_constraint(v, pltpu.HBM) for v in held))
    gate, up, down, router, *scales = written(moved_arrays)
    return (gate.transpose(0, 2, 1), up.transpose(0, 2, 1), down, *scales, router.T)


def solution(mesh):
    torus = Mesh(
        mesh.devices.reshape(2, 2, 4, 4, 2),
        ("expert_0", "expert_1", "shard_0", "shard_1", "shard_2"),
    )
    return jax.shard_map(
        on_device,
        mesh=torus,
        in_specs=(
            P(EXPERT, SHARD, None),
            P(EXPERT, SHARD, None),
            P(EXPERT, None, SHARD),
            P(SHARD, EXPERT),
            P(SHARD),
        ),
        out_specs=(
            P(EXPERT, None, SHARD),
            P(EXPERT, None, SHARD),
            P(EXPERT, SHARD, None),
            P(EXPERT, SHARD),
            P(EXPERT, SHARD),
            P(EXPERT, SHARD),
            P(),
        ),
        check_vma=False,
    )
```

```python
import functools

import jax
import jax.numpy as jnp
from jax import lax
from jax.experimental import pallas as pl
from jax.experimental.pallas import tpu as pltpu
from jax.sharding import Mesh
from jax.sharding import PartitionSpec as P

SHARD = ("shard_0", "shard_1", "shard_2")
EXPERT = ("expert_0", "expert_1")
MESH = pl.DeviceIdType.MESH

ORDER = tuple(
    (a, (a + step) % 4, (a + half) % 2)
    for step in range(4) for half in range(2) for a in range(4)
    if (a, (a + step) % 4, (a + half) % 2) != (0, 0, 0)
)
FAR_FIRST = sorted(range(31), key=lambda k: -sum((0, 1, 2, 1)[v] for v in ORDER[k][:2]) - 2 * ORDER[k][2])
PAIRS = 8
CUT = 4
LAST = 2
CHUNKS = 3 * PAIRS // CUT


def place():
    xl, core, z, y, xh = (lax.axis_index(a) for a in EXPERT + SHARD)
    return xl, core, z, y, xh


def peer(where, offset):
    xl, core, z, y, xh = where
    dz, dy, dx = offset
    turn = 1 - 2 * core
    pz, py, px = (z + turn * dz + 4) % 4, (y + turn * dy + 4) % 4, (xh + dx) % 2
    return (xl, core, pz, py, px), (pz * 4 + py) * 2 + px


def halves(first, second):
    low = jnp.concatenate([first[..., 0:64], second[..., 0:64]], axis=-1)
    high = jnp.concatenate([first[..., 64:128], second[..., 64:128]], axis=-1)
    return low, high


def exchange(
    gate, up, down, router_at, gain_at,
    out_gate, out_up, out_down, out_router, scale_gate, scale_up, scale_down,
    landed, routed, router, gain, rows, part, parts, scale, ready, mine,
    load_sem, sum_send, sum_recv, all_send, all_recv,
    data_send, data_recv, own_sem, r_send, r_recv, g_send, g_recv, r_own,
):
    where = place()
    xl, core, z, y, xh = where
    block = z * 4 + y
    me = block * 2 + xh
    group = xl * 2 + core
    peers = [peer(where, offset) for offset in ORDER]
    planes = [(xl, core, (z + dz) % 4, (y + dy) % 4, xh) for dz in range(4) for dy in range(4) if dz or dy]
    twins = ((xl, 1 - core, z, y, xh), (1 - xl, core, z, y, xh), (1 - xl, core, z, y, 1 - xh))

    loads = [
        pltpu.make_async_copy(source, rows.at[t], load_sem.at[t])
        for t, source in enumerate((gate, up, down))
    ]
    loads[0].start()
    smalls = [
        pltpu.make_async_copy(source, target, load_sem.at[3 + k])
        for k, (source, target) in enumerate(((router_at, router), (gain_at, gain)))
    ]
    for load in smalls:
        load.start()
    barrier = pltpu.get_barrier_semaphore()
    for device, _ in peers:
        pl.semaphore_signal(barrier, inc=1, device_id=device, device_id_type=MESH)
    for device in twins:
        pl.semaphore_signal(barrier, inc=1, device_id=device, device_id_type=MESH)

    for load in smalls:
        load.wait()
    narrow = (router[...] * gain[...]).astype(jnp.bfloat16).astype(jnp.float32)
    mine[...] = jnp.concatenate([narrow[0:8], narrow[8:16]], axis=1).astype(jnp.bfloat16)

    for t in range(3):
        loads[t].wait()
        if t < 2:
            loads[t + 1].start()

        def add_up(e, carry):
            for k in range(8):
                value = rows[t, e, :, pl.ds(k * 128, 128)]
                part[t, e, pl.ds(k, 1), :] = jnp.sum(value * value, axis=0, keepdims=True)
            return carry

        lax.fori_loop(0, 16, add_up, 0)
        if t == 0:
            pl.semaphore_wait(barrier, 34)
        for k, (device, index) in enumerate(peers):
            pltpu.make_async_remote_copy(
                part.at[t, index // 2], parts.at[t, me], sum_send.at[t], sum_recv.at[t],
                device_id=device, device_id_type=MESH,
            ).start()
        parts[t, me] = part[t, block]
        if t == 0:
            for device, _ in peers:
                pltpu.make_async_remote_copy(
                    mine, routed.at[group, me], r_send, r_recv, device_id=device, device_id_type=MESH
                ).start()
            own = pltpu.make_async_copy(mine, routed.at[group, me], r_own)
            own.start()
            own.wait()

    for t in range(3):
        pltpu.make_async_copy(parts.at[t, pl.ds(0, 31)], parts.at[t, pl.ds(0, 31)], sum_recv.at[t]).wait()
        total = parts[t, 0]
        for s in range(1, 32):
            total = total + parts[t, s]
        scale[t, block] = jnp.sqrt(total)
        for device in planes:
            pltpu.make_async_remote_copy(
                scale.at[t, block], scale.at[t, block], all_send.at[t], all_recv.at[t],
                device_id=device, device_id_type=MESH,
            ).start()

    def turned_by(q):
        return [(q * 5 + k) % 31 for k in range(31)]

    def send_out(messages):
        for q, k in messages:
            device, index = peers[k]
            pltpu.make_async_remote_copy(
                ready.at[q, index], landed.at[q, me], data_send.at[q], data_recv.at[q],
                device_id=device, device_id_type=MESH,
            ).start()
        for q in sorted({q for q, _ in messages}):
            pltpu.make_async_copy(ready.at[q, me], landed.at[q, me], own_sem.at[q]).start()

    for t in range(3):
        pltpu.make_async_copy(scale.at[t, pl.ds(0, 15)], scale.at[t, pl.ds(0, 15)], all_recv.at[t]).wait()

        def narrowed(p, carry):
            q = t * (PAIRS // CUT) + p // CUT
            for k in range(8):
                low = rows[t, 2 * p, :, pl.ds(k * 128, 128)] * (1.0 / scale[t, 2 * p, pl.ds(k, 1), :])
                high = rows[t, 2 * p + 1, :, pl.ds(k * 128, 128)] * (1.0 / scale[t, 2 * p + 1, pl.ds(k, 1), :])
                both = jnp.concatenate([low, high], axis=0)
                ready[q, pl.ds(4 * k, 4), p % CUT] = both.T.astype(jnp.bfloat16).reshape(4, 32, 128)
            return carry

        for part_of in range(PAIRS // CUT):
            q = t * (PAIRS // CUT) + part_of
            lax.fori_loop(part_of * CUT, part_of * CUT + CUT, narrowed, 0)
            if q < CHUNKS - LAST:
                send_out([(q, k) for k in turned_by(q)])
            elif q == CHUNKS - 1:
                send_out([(r, k) for k in FAR_FIRST for r in range(CHUNKS - LAST, CHUNKS)])
        rolled = pltpu.roll(scale[t, :, me // 4, :], (128 - 32 * (me % 4)) % 128, 1)
        (scale_gate, scale_up, scale_down)[t][...] = rolled[:, 0:32]
        if t == 0:
            pltpu.make_async_copy(routed.at[group, pl.ds(0, 31)], routed.at[group, pl.ds(0, 31)], r_recv).wait()
            pltpu.make_async_remote_copy(
                routed.at[group], routed.at[group], g_send.at[0], g_recv.at[0], device_id=twins[0], device_id_type=MESH
            ).start()
            for k in range(2):
                half = routed.at[group, pl.ds(16 * k, 16)]
                pltpu.make_async_remote_copy(
                    half, half, g_send.at[1 + k], g_recv.at[1 + k], device_id=twins[1 + k], device_id_type=MESH
                ).start()
        if t == 1:
            for k in (1, 2):
                pltpu.make_async_copy(routed.at[0, pl.ds(0, 16)], routed.at[0, pl.ds(0, 16)], g_recv.at[k]).wait()
            other = (1 - xl) * 2 + core
            pltpu.make_async_remote_copy(
                routed.at[other], routed.at[other], g_send.at[3], g_recv.at[3], device_id=twins[0], device_id_type=MESH
            ).start()

    for t, out in enumerate((out_gate, out_up, out_down)):
        for part_of in range(PAIRS // CUT):
            q = t * (PAIRS // CUT) + part_of
            pltpu.make_async_copy(ready.at[q, me], landed.at[q, me], own_sem.at[q]).wait()
            pltpu.make_async_copy(ready.at[q, pl.ds(0, 31)], ready.at[q, pl.ds(0, 31)], data_recv.at[q]).wait()

            def put(p, carry):
                for k in range(16):
                    low, high = halves(landed[q, 2 * k, p], landed[q, 2 * k + 1, p])
                    expert = 2 * (part_of * CUT + p)
                    out[expert, :, pl.ds(k * 128, 128)] = low
                    out[expert + 1, :, pl.ds(k * 128, 128)] = high
                return carry

            lax.fori_loop(0, CUT, put, 0)
        if t == 1:
            for k in (0, 3):
                pltpu.make_async_copy(routed.at[0], routed.at[0], g_recv.at[k]).wait()

            def put_router(g, carry):
                for k in range(16):
                    low, high = halves(routed[g, 2 * k], routed[g, 2 * k + 1])
                    out_router[pl.ds(pl.multiple_of(16 * g, 16), 16), pl.ds(k * 128, 128)] = jnp.concatenate([low, high], axis=0)
                return carry

            lax.fori_loop(0, 4, put_router, 0)

    for k in (0, 3):
        pltpu.make_async_copy(routed.at[0], routed.at[0], g_send.at[k]).wait()
    for k in (1, 2):
        pltpu.make_async_copy(routed.at[0, pl.ds(0, 16)], routed.at[0, pl.ds(0, 16)], g_send.at[k]).wait()
    pltpu.make_async_copy(routed.at[0, pl.ds(0, 31)], routed.at[0, pl.ds(0, 31)], r_send).wait()
    for t in range(3):
        pltpu.make_async_copy(parts.at[t, pl.ds(0, 31)], parts.at[t, pl.ds(0, 31)], sum_send.at[t]).wait()
        pltpu.make_async_copy(scale.at[t, pl.ds(0, 15)], scale.at[t, pl.ds(0, 15)], all_send.at[t]).wait()
    for q in range(CHUNKS):
        pltpu.make_async_copy(ready.at[q, pl.ds(0, 31)], ready.at[q, pl.ds(0, 31)], data_send.at[q]).wait()


def moved(gate, up, down, router, gain):
    hbm = pl.BlockSpec(memory_space=pl.ANY)
    vmem = pl.BlockSpec(memory_space=pltpu.VMEM)
    dma = pltpu.SemaphoreType.DMA
    return pl.pallas_call(
        exchange,
        name="exchange",
        out_shape=tuple(pltpu.VMEM((16, 32, 2048), jnp.bfloat16) for _ in range(3))
        + (pltpu.VMEM((64, 2048), jnp.bfloat16),)
        + tuple(pltpu.VMEM((16, 32), jnp.float32) for _ in range(3)),
        in_specs=[hbm] * 5,
        out_specs=(vmem,) * 7,
        scratch_shapes=[
            pltpu.VMEM((CHUNKS, 32, CUT, 32, 128), jnp.bfloat16),
            pltpu.VMEM((4, 32, 8, 128), jnp.bfloat16),
            pltpu.VMEM((16, 64), jnp.float32),
            pltpu.VMEM((1, 64), jnp.float32),
            pltpu.VMEM((3, 16, 64, 1024), jnp.float32),
            pltpu.VMEM((3, 16, 8, 128), jnp.float32),
            pltpu.VMEM((3, 32, 8, 128), jnp.float32),
            pltpu.VMEM((3, 16, 8, 128), jnp.float32),
            pltpu.VMEM((CHUNKS, 32, CUT, 32, 128), jnp.bfloat16),
            pltpu.VMEM((8, 128), jnp.bfloat16),
            dma((5,)), dma((3,)), dma((3,)), dma((3,)), dma((3,)),
            dma((CHUNKS,)), dma((CHUNKS,)), dma((CHUNKS,)),
            dma, dma, dma((4,)), dma((4,)), dma,
        ],
        compiler_params=pltpu.CompilerParams(collective_id=0, has_side_effects=True, vmem_limit_bytes=54 * 2**20),
    )(gate, up, down, router, gain)


def write_out(*refs):
    sources, targets, sem = refs[:7], refs[7:14], refs[14]
    copies = [pltpu.make_async_copy(sources[k], targets[k], sem.at[k]) for k in range(7)]
    for copy in copies:
        copy.start()
    for copy in copies:
        copy.wait()


def written(arrays):
    hbm = pl.BlockSpec(memory_space=pltpu.HBM)
    vmem = pl.BlockSpec(memory_space=pltpu.VMEM)
    return pl.pallas_call(
        write_out,
        name="write_out",
        out_shape=tuple(jax.ShapeDtypeStruct(v.shape, v.dtype) for v in arrays),
        in_specs=[vmem] * 7,
        out_specs=(hbm,) * 7,
        scratch_shapes=[pltpu.SemaphoreType.DMA((7,))],
        compiler_params=pltpu.CompilerParams(vmem_limit_bytes=2**20),
    )(*(pltpu.with_memory_space_constraint(v, pltpu.VMEM) for v in arrays))


def on_device(master_gate, master_up, master_down, router_weight, router_gain):
    held = (master_gate, master_up, master_down.transpose(0, 2, 1), router_weight.T, router_gain.reshape(1, 64))
    moved_arrays = moved(*(pltpu.with_memory_space_constraint(v, pltpu.HBM) for v in held))
    gate, up, down, router, *scales = written(moved_arrays)
    return (gate.transpose(0, 2, 1), up.transpose(0, 2, 1), down, *scales, router.T)


def solution(mesh):
    torus = Mesh(
        mesh.devices.reshape(2, 2, 4, 4, 2),
        ("expert_0", "expert_1", "shard_0", "shard_1", "shard_2"),
    )
    return jax.shard_map(
        on_device,
        mesh=torus,
        in_specs=(
            P(EXPERT, SHARD, None),
            P(EXPERT, SHARD, None),
            P(EXPERT, None, SHARD),
            P(SHARD, EXPERT),
            P(SHARD),
        ),
        out_specs=(
            P(EXPERT, None, SHARD),
            P(EXPERT, None, SHARD),
            P(EXPERT, SHARD, None),
            P(EXPERT, SHARD),
            P(EXPERT, SHARD),
            P(EXPERT, SHARD),
            P(),
        ),
        check_vma=False,
    )
```
